32 devices in a mesh: gx: 4 (over z), gy: 2 (over y), gz: 4 (over x, core).
Axes of the slice: x: 2, y: 2, z: 4, core: 2. Of those that a mesh axis runs over, the one named last changes fastest.
Arguments:
- acts: bfloat16 [18816, 2048], P(('gx', 'gy', 'gz')), may hold values from -6 to 6
- saved_hidden: bfloat16 [18816, 512], P(('gx', 'gy', 'gz')), as said below
- grad_out: bfloat16 [18816, 2048], P(('gx', 'gy', 'gz')), may hold values from -6 to 6
- master_reduce: float32 [2048, 512], P(('gx', 'gy', 'gz')), may hold values from -60 to 60
- master_expand: float32 [2048, 512], P(('gx', 'gy', 'gz')), may hold values from -60 to 60
- velocity_reduce: float32 [2048, 512], P(('gx', 'gy', 'gz')), may hold values from -6 to 6
- velocity_expand: float32 [2048, 512], P(('gx', 'gy', 'gz')), may hold values from -6 to 6
Outputs:
- grad_in: bfloat16 [18816, 2048], P(('gx', 'gy', 'gz'))
- new_master_reduce: float32 [2048, 512], P(('gx', 'gy', 'gz'))
- new_master_expand: float32 [2048, 512], P(('gx', 'gy', 'gz'))
- new_velocity_reduce: float32 [2048, 512], P(('gx', 'gy', 'gz'))
- new_velocity_expand: float32 [2048, 512], P(('gx', 'gy', 'gz'))
- work_reduce: bfloat16 [2048, 512], replicated
- work_expand: bfloat16 [2048, 512], replicated
The draws below stay inside these ranges and needn't reach their ends.
Inputs may be any that keep to these rules, and one draw needn't show every extreme that they name: `saved_hidden`: values are zero or positive, zero at about half of the entries.
All inputs are finite; a program needn't handle non-finite values.
Results may differ from the reference program's by a relative error of at most 0.0064.
Values may be sent and summed in bfloat16 or wider, within the bound.
A program may use at most 64 MiB of HBM per device.

```python
import jax
import jax.numpy as jnp
from jax import lax

CHANNELS = 2048
MIDDLE = 512
ROWS = 18816


def draw_saved_hidden(key, part):
    values = jax.random.normal(jax.random.fold_in(key, 11), (ROWS, MIDDLE), jnp.float32)
    return jnp.maximum(values, 0.0).astype(jnp.bfloat16)


def rising_master(key, salt):
    values = jnp.clip(jax.random.normal(jax.random.fold_in(key, salt), (CHANNELS, MIDDLE), jnp.float32), -6.0, 6.0)
    place = jnp.arange(CHANNELS, dtype=jnp.float32)[:, None] / float(max(CHANNELS - 1, 1))
    scales = 1.0 + 2.0 * place
    return values * scales


def draw_master_reduce(key, part):
    return rising_master(key, 21)


def draw_master_expand(key, part):
    return rising_master(key, 31)


def strengthened(entries, stream_key, source, target, shards_of, factor):
    owner, partner = [(jnp.arange(entries.shape[dim]) // (entries.shape[dim] // shards_of)).reshape([-1 if axis == dim else 1 for axis in range(entries.ndim)]) for dim in (source, target)]
    chosen = jax.random.permutation(stream_key, shards_of)[partner]
    strong = (owner == chosen) | (owner == (partner + shards_of // 2) % shards_of)
    return jnp.where(strong, factor * entries, entries)


def levels(key, extent, cuts, least, high):
    def one(dim, shards_of):
        steps = jax.random.uniform(jax.random.fold_in(jax.random.fold_in(key, 6), dim), (shards_of,), jnp.float32, least / len(cuts), high / len(cuts))
        return jnp.repeat(jnp.exp(steps), extent[dim] // shards_of).reshape((-1,) + (1,) * (len(extent) - dim - 1))

    level = one(*cuts[0])
    for cut in cuts[1:]:
        level = level * one(*cut)
    return level


def gaussian(rng, dims, deviation, most, cuts=(), held_as=jnp.bfloat16):
    level = levels(rng, dims, cuts, -0.22, 0.18) if cuts else 1.0
    entries = jax.random.normal(rng, dims, jnp.float32) * deviation * level
    return jnp.minimum(jnp.maximum(entries, -most), most).astype(held_as)


def gaussian_with(rng, extent, scale, most, split, heavy, held_as=jnp.bfloat16):
    drawn = scale * jax.random.normal(rng, extent, jnp.float32)
    if split:
        drawn = drawn * levels(rng, extent, split, -0.22, 0.18)
    return jnp.clip(strengthened(drawn, jax.random.fold_in(rng, 3), *heavy), -most, most).astype(held_as)


def setup_inputs(seed: int = 0) -> dict:
    key_list = jax.random.split(jax.random.key(seed), 8)
    return {
        "acts": gaussian_with(key_list[0], (ROWS, CHANNELS), 1.0, 6.0, ((0, 32),), (0, 1, 32, 2.75)),
        "saved_hidden": draw_saved_hidden(jax.random.fold_in(key_list[7], 71), 0),
        "grad_out": gaussian_with(key_list[2], (ROWS, CHANNELS), 1.0, 6.0, ((0, 32),), (0, 1, 32, 2.75)),
        "master_reduce": draw_master_reduce(jax.random.fold_in(key_list[7], 71), 0),
        "master_expand": draw_master_expand(jax.random.fold_in(key_list[7], 71), 0),
        "velocity_reduce": gaussian(key_list[5], (CHANNELS, MIDDLE), 1.0, 6.0, ((0, 32),), jnp.float32),
        "velocity_expand": gaussian(key_list[6], (CHANNELS, MIDDLE), 1.0, 6.0, ((0, 32),), jnp.float32),
    }


def layer_update(master, grads, velocity):
    wnorm = jnp.sqrt(jnp.sum(master * master))
    gnorm = jnp.sqrt(jnp.sum(grads * grads))
    trust = wnorm / (gnorm + 5e-05 * wnorm)
    new_velocity = 0.9 * velocity + trust * (grads + 5e-05 * master)
    new_master = master - 0.1 * new_velocity
    return (new_master, new_velocity, new_master.astype(jnp.bfloat16))

def reference(acts, saved_hidden, grad_out, master_reduce, master_expand, velocity_reduce, velocity_expand):
    inv_c = 1.0 / math_sqrt(CHANNELS)
    inv_m = 1.0 / math_sqrt(MIDDLE)
    cur_reduce = master_reduce.astype(jnp.bfloat16)
    cur_expand = master_expand.astype(jnp.bfloat16)
    summed = jnp.dot(grad_out, cur_expand, preferred_element_type=jnp.float32)
    grad_hidden = jnp.where(saved_hidden > 0, summed * inv_m, 0.0).astype(jnp.bfloat16)
    g_expand = lax.dot_general(grad_out, saved_hidden, (((0,), (0,)), ((), ())), preferred_element_type=jnp.float32) * inv_m
    g_reduce = lax.dot_general(acts, grad_hidden, (((0,), (0,)), ((), ())), preferred_element_type=jnp.float32) * inv_c
    back = lax.dot_general(grad_hidden, cur_reduce, (((1,), (1,)), ((), ())), preferred_element_type=jnp.float32)
    grad_in = (grad_out.astype(jnp.float32) + back * inv_c).astype(jnp.bfloat16)
    new_mr, new_vr, work_reduce = layer_update(master_reduce, g_reduce, velocity_reduce)
    new_me, new_ve, work_expand = layer_update(master_expand, g_expand, velocity_expand)
    return (grad_in, new_mr, new_me, new_vr, new_ve, work_reduce, work_expand)

def math_sqrt(value):
    return float(value) ** 0.5
```

```python
import functools

import jax
import jax.numpy as jnp
from jax import lax
from jax.experimental import pallas as pl
from jax.experimental.pallas import tpu as pltpu
from jax.sharding import PartitionSpec as P

AXES = ("gx", "gy", "gz")
MESH = pl.DeviceIdType.MESH
SLABS = 2


class Plan:
    def __init__(self, shape):
        self.sizes = dict(shape)
        self.factors = []
        for axis in reversed(AXES):
            stride = 1
            while stride < self.sizes[axis]:
                self.factors.append((axis, stride))
                stride *= 2
            assert stride == self.sizes[axis]
        self.n = len(self.factors)

    def order(self, slab):
        order = list(range(self.n))
        if slab % 2 and self.n > 2:
            order[1], order[2] = order[2], order[1]
        return order

    def digits(self):
        me = {a: lax.axis_index(a) for a in AXES}
        digits = [lax.rem(me[a] // s, 2) for a, s in self.factors]
        peers = [{a: me[a] + (1 - 2 * d) * s} for (a, s), d in zip(self.factors, digits)]
        return digits, peers

    def axis_peers(self, axis):
        me, n = lax.axis_index(axis), self.sizes[axis]
        return [{axis: lax.rem(me + j, n)} for j in range(1, n)]


def enter(plan):
    barrier = pltpu.get_barrier_semaphore()
    count = 0
    for axis in AXES:
        for peer in plan.axis_peers(axis):
            pl.semaphore_signal(barrier, inc=1, device_id=peer, device_id_type=MESH)
            count += 1
    pl.semaphore_wait(barrier, count)


def remote(src, dst, send, recv, peer):
    return pltpu.make_async_remote_copy(
        src_ref=src, dst_ref=dst, send_sem=send, recv_sem=recv,
        device_id=peer, device_id_type=MESH,
    )


def gather_stage(plan, digits, peers, t, stream, work, send, recv):
    layer, slab = stream
    order = plan.order(slab)
    held = order[t + 1 :]
    region = tuple(
        slice(None) if k in held else digits[k] for k in reversed(range(plan.n))
    )
    cols = work[layer].shape[-1] // SLABS
    part = work[layer].at[region + (slice(None), pl.ds(slab * cols, cols))]
    at = layer * SLABS + slab
    return remote(part, part, send.at[t, at], recv.at[t, at], peers[order[t]])


def gather(plan, digits, peers, streams, work, send, recv):
    copies = {}
    for t in reversed(range(plan.n)):
        for stream in streams:
            if t < plan.n - 1:
                copies[t + 1, stream].wait_recv()
            copy = gather_stage(plan, digits, peers, t, stream, work, send, recv)
            copy.start()
            copies[t, stream] = copy
    for stream in streams:
        copies[0, stream].wait_recv()
    for copy in copies.values():
        copy.wait_send()


def own_block(plan, digits):
    return tuple(digits[k] for k in reversed(range(plan.n)))


def gather_kernel(plan, mr, me, work_r, work_e, send, recv):
    digits, peers = plan.digits()
    own = own_block(plan, digits)
    work_r[own] = mr[...].astype(jnp.bfloat16)
    work_e[own] = me[...].astype(jnp.bfloat16)
    enter(plan)
    streams = [(layer, slab) for layer in (1, 0) for slab in range(SLABS)]
    gather(plan, digits, peers, streams, (work_r, work_e), send, recv)


def update_kernel(
    plan, pr, pe, mr, me, vr, ve,
    new_mr, new_me, new_vr, new_ve, work_r, work_e,
    total, sends, recvs, sums, shares, grads,
    rs_send, rs_recv, ag_send, ag_recv, n_send, n_recv,
):
    digits, peers = plan.digits()
    enter(plan)
    partial = (pr, pe)
    cols = pr.shape[-1] // SLABS
    streams = [(layer, slab) for layer in (0, 1) for slab in range(SLABS)]
    copies = {}
    last = plan.n - 1

    def position(order, t):
        rem = [k for k in reversed(range(plan.n)) if k not in order[:t]]
        at = rem.index(order[t])
        return 2 ** (len(rem) - at - 1)

    def kept(stream, t, bit, i):
        layer, slab = stream
        post = position(plan.order(slab), t)
        at = (i // post * 2 + bit) * post + i % post
        if t == 0:
            return partial[layer][at, :, pl.ds(slab * cols, cols)]
        return total[t - 1][layer * SLABS + slab, at]

    for t in range(plan.n):
        blocks = 2 ** (plan.n - t - 1)
        for stream in streams:
            layer, slab = stream
            s = layer * SLABS + slab
            order = plan.order(slab)
            if t > 0:
                copies[t - 1, s].wait_recv()
                before = digits[order[t - 1]]

                def add(i, c, stream=stream, s=s, t=t, before=before):
                    total[t - 1][s, i] = kept(stream, t - 1, before, i) + recvs[t - 1][
                        s, i
                    ].astype(jnp.float32)
                    return c

                lax.fori_loop(0, 2 * blocks, add, 0)
            away = 1 - digits[order[t]]

            def pack(i, c, stream=stream, s=s, t=t, away=away):
                sends[t][s, i] = kept(stream, t, away, i).astype(jnp.bfloat16)
                return c

            lax.fori_loop(0, blocks, pack, 0)
            copy = remote(
                sends[t].at[s], recvs[t].at[s], rs_send.at[t, s], rs_recv.at[t, s],
                peers[order[t]],
            )
            copy.start()
            copies[t, s] = copy

    for stream in streams:
        layer, slab = stream
        s = layer * SLABS + slab
        copies[last, s].wait_recv()
        grads[layer, :, pl.ds(slab * cols, cols)] = kept(
            stream, last, digits[plan.order(slab)[last]], 0
        ) + recvs[last][s, 0].astype(jnp.float32)

    def square(x):
        x = x * x
        lanes = jnp.sum(x, axis=0, keepdims=True)
        width = lanes.shape[1]
        return sum(lanes[:, c : c + 128] for c in range(0, width, 128))

    rows = [square(mr[...]), square(grads[0]), square(me[...]), square(grads[1])]
    sums[0] = jnp.concatenate(rows + [jnp.zeros((4, 128), jnp.float32)], axis=0)
    small, slot = [], 0
    for a, axis in enumerate(AXES):
        mine = []
        for peer in plan.axis_peers(axis):
            copy = remote(sums.at[a], shares.at[slot], n_send.at[slot], n_recv.at[slot], peer)
            copy.start()
            mine.append((copy, slot))
            slot += 1
        whole = sums[a]
        for copy, at in mine:
            copy.wait_recv()
            whole = whole + shares[at]
        sums[a + 1] = whole
        small += [copy for copy, _ in mine]
    stats = jnp.sum(sums[len(AXES)], axis=1, keepdims=True)

    own = own_block(plan, digits)
    for layer, (m, v, out_m, out_v, work) in enumerate(
        ((mr, vr, new_mr, new_vr, work_r), (me, ve, new_me, new_ve, work_e))
    ):
        wnorm = jnp.sqrt(stats[2 * layer : 2 * layer + 1])
        gnorm = jnp.sqrt(stats[2 * layer + 1 : 2 * layer + 2])
        trust = wnorm / (gnorm + 5e-05 * wnorm)
        velocity = 0.9 * v[...] + trust * (grads[layer] + 5e-05 * m[...])
        master = m[...] - 0.1 * velocity
        out_v[...] = velocity
        out_m[...] = master
        work[own] = master.astype(jnp.bfloat16)

    gather(plan, digits, peers, streams, (work_r, work_e), ag_send, ag_recv)
    for copy in list(copies.values()) + small:
        copy.wait_send()


VMEM = pl.BlockSpec(memory_space=pltpu.VMEM)


def all_gathered(plan, mr, me):
    rows, width = mr.shape
    shape = jax.ShapeDtypeStruct((2,) * plan.n + (rows, width), jnp.bfloat16)
    sems = pltpu.SemaphoreType.DMA((plan.n, 2 * SLABS))
    out = pl.pallas_call(
        functools.partial(gather_kernel, plan),
        out_shape=(shape, shape),
        in_specs=[VMEM] * 2,
        out_specs=(VMEM, VMEM),
        scratch_shapes=[sems, sems],
        compiler_params=pltpu.CompilerParams(collective_id=0, has_side_effects=True),
        name="gather_weights",
    )(mr, me)
    return [x.reshape(-1, width) for x in out]


def updated(plan, pr, pe, mr, me, vr, ve):
    rows, width = mr.shape
    n, streams = plan.n, 2 * SLABS
    cols = width // SLABS
    f32, bf16 = jnp.float32, jnp.bfloat16
    work = jax.ShapeDtypeStruct((2,) * n + (rows, width), bf16)
    shard = jax.ShapeDtypeStruct((rows, width), f32)
    sems = pltpu.SemaphoreType.DMA((n, streams))
    slots = sum(plan.sizes[a] - 1 for a in AXES)
    half = [2 ** (n - t - 1) for t in range(n)]
    out = pl.pallas_call(
        functools.partial(update_kernel, plan),
        out_shape=(shard,) * 4 + (work,) * 2,
        in_specs=[VMEM] * 6,
        out_specs=(VMEM,) * 6,
        scratch_shapes=[
            [pltpu.VMEM((streams, b, rows, cols), f32) for b in half],
            [pltpu.VMEM((streams, b, rows, cols), bf16) for b in half],
            [pltpu.VMEM((streams, b, rows, cols), bf16) for b in half],
            pltpu.VMEM((len(AXES) + 1, 8, 128), f32),
            pltpu.VMEM((slots, 8, 128), f32),
            pltpu.VMEM((2, rows, width), f32),
            sems, sems, sems, sems,
            pltpu.SemaphoreType.DMA((slots,)),
            pltpu.SemaphoreType.DMA((slots,)),
        ],
        compiler_params=pltpu.CompilerParams(collective_id=1, has_side_effects=True),
        name="reduce_update_gather",
    )(pr.reshape(-1, rows, width), pe.reshape(-1, rows, width), mr, me, vr, ve)
    return out[:4] + tuple(x.reshape(-1, width) for x in out[4:])


def shards(
    plan, acts, saved_hidden, grad_out, master_reduce, master_expand,
    velocity_reduce, velocity_expand,
):
    inv_c = 1.0 / float(grad_out.shape[1]) ** 0.5
    inv_m = 1.0 / float(saved_hidden.shape[1]) ** 0.5
    f32 = jnp.float32
    cur_reduce, cur_expand = all_gathered(plan, master_reduce, master_expand)
    summed = jnp.dot(grad_out, cur_expand, preferred_element_type=f32)
    grad_hidden = jnp.where(saved_hidden > 0, summed * inv_m, 0.0).astype(jnp.bfloat16)
    over_rows = (((0,), (0,)), ((), ()))
    g_expand = lax.dot_general(grad_out, saved_hidden, over_rows, preferred_element_type=f32) * inv_m
    g_reduce = lax.dot_general(acts, grad_hidden, over_rows, preferred_element_type=f32) * inv_c
    back = lax.dot_general(
        grad_hidden, cur_reduce, (((1,), (1,)), ((), ())), preferred_element_type=f32
    )
    grad_in = (grad_out.astype(f32) + back * inv_c).astype(jnp.bfloat16)
    new_mr, new_me, new_vr, new_ve, work_reduce, work_expand = updated(
        plan, g_reduce, g_expand, master_reduce, master_expand, velocity_reduce, velocity_expand
    )
    return (grad_in, new_mr, new_me, new_vr, new_ve, work_reduce, work_expand)


def solution(mesh):
    rows = P(AXES, None)
    return jax.shard_map(
        functools.partial(shards, Plan(mesh.shape)),
        mesh=mesh,
        in_specs=(rows,) * 7,
        out_specs=(rows,) * 5 + (P(), P()),
        check_vma=False,
    )
```

```python
import functools

import jax
import jax.numpy as jnp
from jax import lax
from jax.experimental import pallas as pl
from jax.experimental.pallas import tpu as pltpu
from jax.sharding import PartitionSpec as P

AXES = ("gx", "gy", "gz")
MESH = pl.DeviceIdType.MESH
SLABS = 2


class Plan:
    def __init__(self, shape):
        self.sizes = dict(shape)
        self.factors = []
        for axis in reversed(AXES):
            stride = 1
            while stride < self.sizes[axis]:
                self.factors.append((axis, stride))
                stride *= 2
            assert stride == self.sizes[axis]
        self.n = len(self.factors)

    def order(self, slab):
        order = list(range(self.n))
        if slab % 2 and self.n > 2:
            order[1], order[2] = order[2], order[1]
        return order

    def digits(self):
        me = {a: lax.axis_index(a) for a in AXES}
        digits = [lax.rem(me[a] // s, 2) for a, s in self.factors]
        peers = [{a: me[a] + (1 - 2 * d) * s} for (a, s), d in zip(self.factors, digits)]
        return digits, peers

    def axis_peers(self, axis):
        me, n = lax.axis_index(axis), self.sizes[axis]
        return [{axis: lax.rem(me + j, n)} for j in range(1, n)]


def enter(plan):
    barrier = pltpu.get_barrier_semaphore()
    count = 0
    for axis in AXES:
        for peer in plan.axis_peers(axis):
            pl.semaphore_signal(barrier, inc=1, device_id=peer, device_id_type=MESH)
            count += 1
    pl.semaphore_wait(barrier, count)


def remote(src, dst, send, recv, peer):
    return pltpu.make_async_remote_copy(
        src_ref=src, dst_ref=dst, send_sem=send, recv_sem=recv,
        device_id=peer, device_id_type=MESH,
    )


def own_block(plan, digits):
    return tuple(digits[k] for k in reversed(range(plan.n)))


def position(plan, order, t):
    rem = [k for k in reversed(range(plan.n)) if k not in order[:t]]
    return 2 ** (len(rem) - rem.index(order[t]) - 1)


class Gather:
    def __init__(self, plan, slab, where, work, send, recv, used):
        self.plan, self.slab, self.where, self.work = plan, slab, where, work
        self.send, self.recv, self.used = send, recv, used
        self.t, self.copy = plan.n - 1, None

    def step(self):
        assert self.t >= -1
        if self.copy is not None:
            self.copy.wait_recv()
        if self.t < 0:
            self.t = -2
            return
        digits, peers = self.where
        plan, t = self.plan, self.t
        order = plan.order(self.slab)
        held = order[t + 1 :]
        region = tuple(
            slice(None) if k in held else digits[k] for k in reversed(range(plan.n))
        )
        cols = self.work.shape[-1] // SLABS
        part = self.work.at[region + (slice(None), pl.ds(self.slab * cols, cols))]
        self.copy = remote(
            part, part, self.send.at[t, self.slab], self.recv.at[t, self.slab], peers[order[t]]
        )
        self.copy.start()
        self.used.append(self.copy)
        self.t = t - 1


class Scatter:
    def __init__(self, plan, slab, where, partial, total, sends, recvs, grad, send, recv, used):
        self.plan, self.slab, self.where, self.partial = plan, slab, where, partial
        self.total, self.sends, self.recvs, self.grad = total, sends, recvs, grad
        self.send, self.recv, self.used = send, recv, used
        self.t, self.copy = 0, None
        self.cols = partial.shape[-1] // SLABS

    def kept(self, t, bit, i):
        post = position(self.plan, self.plan.order(self.slab), t)
        at = (i // post * 2 + bit) * post + i % post
        if t == 0:
            return self.partial[at, :, pl.ds(self.slab * self.cols, self.cols)]
        return self.total[t - 1][self.slab, at]

    def step(self):
        digits, peers = self.where
        plan, t, s = self.plan, self.t, self.slab
        order = plan.order(s)
        sends, recvs, total = self.sends, self.recvs, self.total
        if t > 0:
            self.copy.wait_recv()
            before = digits[order[t - 1]]

            def summed(i):
                return self.kept(t - 1, before, i) + recvs[t - 1][s, i].astype(jnp.float32)

            if t == plan.n:
                self.grad[:, pl.ds(s * self.cols, self.cols)] = summed(0)
                return

            def add(i, c):
                total[t - 1][s, i] = summed(i)
                return c

            lax.fori_loop(0, 2 ** (plan.n - t), add, 0)
        away = 1 - digits[order[t]]

        def pack(i, c):
            sends[t][s, i] = self.kept(t, away, i).astype(jnp.bfloat16)
            return c

        lax.fori_loop(0, 2 ** (plan.n - t - 1), pack, 0)
        self.copy = remote(
            sends[t].at[s], recvs[t].at[s], self.send.at[t, s], self.recv.at[t, s],
            peers[order[t]],
        )
        self.copy.start()
        self.used.append(self.copy)
        self.t = t + 1


class Norms:
    def __init__(self, plan, sums, shares, send, recv, used):
        self.plan, self.sums, self.shares = plan, sums, shares
        self.send, self.recv, self.used = send, recv, used
        self.a, self.slot, self.mine = 0, 0, []

    def begin(self, m, g):
        def square(x):
            x = x * x
            lanes = jnp.sum(x, axis=0, keepdims=True)
            return sum(lanes[:, c : c + 128] for c in range(0, lanes.shape[1], 128))

        rows = [square(m), square(g), jnp.zeros((6, 128), jnp.float32)]
        self.sums[0] = jnp.concatenate(rows, axis=0)
        self.step()

    def step(self):
        if self.mine:
            whole = self.sums[self.a - 1]
            for copy, at in self.mine:
                copy.wait_recv()
                whole = whole + self.shares[at]
            self.sums[self.a] = whole
        self.mine = []
        if self.a == len(AXES):
            return
        for peer in self.plan.axis_peers(AXES[self.a]):
            copy = remote(
                self.sums.at[self.a], self.shares.at[self.slot],
                self.send.at[self.slot], self.recv.at[self.slot], peer,
            )
            copy.start()
            self.used.append(copy)
            self.mine.append((copy, self.slot))
            self.slot += 1
        self.a += 1

    def trust(self):
        stats = jnp.sum(self.sums[len(AXES)], axis=1, keepdims=True)
        wnorm, gnorm = jnp.sqrt(stats[0:1]), jnp.sqrt(stats[1:2])
        return wnorm / (gnorm + 5e-05 * wnorm)


def kernel(
    plan, acts, hidden, grad_out, mr, me, vr, ve,
    grad_hidden, cur_r, new_mr, new_me, new_vr, new_ve, work_r, work_e,
    cur_e, partial_r, partial_e, total_r, total_e, sends_r, sends_e, recvs_r, recvs_e,
    grad_r, grad_e, sums_r, sums_e, shares_r, shares_e,
    g_send, g_recv, s_send, s_recv, n_send, n_recv,
):
    where = digits, _ = plan.digits()
    own = own_block(plan, digits)
    used = []
    width = mr.shape[1]
    rows = mr.shape[0]
    channels = grad_out.shape[1]
    f32 = jnp.float32
    inv_c = 1.0 / float(channels) ** 0.5
    inv_m = 1.0 / float(width) ** 0.5

    def gathers(at, work):
        return [
            Gather(plan, s, where, work, g_send.at[at], g_recv.at[at], used)
            for s in range(SLABS)
        ]

    def scatters(at, partial, total, sends, recvs, grad):
        return [
            Scatter(
                plan, s, where, partial, total, sends, recvs, grad,
                s_send.at[at], s_recv.at[at], used,
            )
            for s in range(SLABS)
        ]

    gather_e, gather_r = gathers(0, cur_e), gathers(1, cur_r)
    final_e, final_r = gathers(2, work_e), gathers(3, work_r)
    scatter_e = scatters(0, partial_e, total_e, sends_e, recvs_e, grad_e)
    scatter_r = scatters(1, partial_r, total_r, sends_r, recvs_r, grad_r)
    norms_e = Norms(plan, sums_e, shares_e, n_send.at[0], n_recv.at[0], used)
    norms_r = Norms(plan, sums_r, shares_r, n_send.at[1], n_recv.at[1], used)

    def step(*groups):
        for group in groups:
            for task in group:
                task.step()

    pieces = 8
    wide = channels // pieces
    over_rows = (((0,), (0,)), ((), ()))

    def weight_grad(left, right, partial, scale, first, count):
        def piece(i, c):
            cols = left[:, pl.ds(pl.multiple_of(i * wide, wide), wide)]
            product = lax.dot_general(cols, right[...], over_rows, preferred_element_type=f32)
            blocks = wide // rows
            partial[pl.ds(i * blocks, blocks)] = (product * scale).reshape(blocks, rows, width)
            return c

        lax.fori_loop(first, first + count, piece, 0)

    def hidden_grad():
        cols = width // 2
        for c in range(0, width, cols):
            weights = cur_e[(slice(None),) * plan.n + (slice(None), pl.ds(c, cols))]
            summed = jnp.dot(
                grad_out[...], weights.reshape(channels, cols), preferred_element_type=f32
            )
            kept = hidden[:, c : c + cols].astype(f32) > 0
            grad_hidden[:, c : c + cols] = jnp.where(kept, summed * inv_m, 0.0).astype(
                jnp.bfloat16
            )

    def update(m, v, out_m, out_v, work, grad, norms):
        velocity = 0.9 * v[...] + norms.trust() * (grad[...] + 5e-05 * m[...])
        master = m[...] - 0.1 * velocity
        out_v[...] = velocity
        out_m[...] = master
        work[own] = master.astype(jnp.bfloat16)

    cur_r[own] = mr[...].astype(jnp.bfloat16)
    cur_e[own] = me[...].astype(jnp.bfloat16)
    enter(plan)

    step(gather_e)
    weight_grad(grad_out, hidden, partial_e, inv_m, 0, pieces // 4)
    step(gather_e, gather_r)
    weight_grad(grad_out, hidden, partial_e, inv_m, pieces // 4, pieces // 4)
    step(gather_e, gather_r)
    weight_grad(grad_out, hidden, partial_e, inv_m, pieces // 2, pieces // 2)
    step(scatter_e)
    for _ in range(plan.n - 3):
        step(gather_e)
    step(scatter_e)
    step(gather_e)
    hidden_grad()
    step(gather_r)
    weight_grad(acts, grad_hidden, partial_r, inv_c, 0, pieces)
    step(scatter_r)
    step(scatter_e)
    step(scatter_r)
    for _ in range(plan.n - 3):
        step(gather_r)
    for _ in range(plan.n - 2):
        step(scatter_e)
    norms_e.begin(me[...], grad_e[...])
    step(scatter_r)
    norms_e.step()
    step(gather_r)
    norms_e.step()
    step(scatter_r)
    norms_e.step()
    update(me, ve, new_me, new_ve, work_e, grad_e, norms_e)
    step(final_e)
    for _ in range(plan.n - 3):
        step(scatter_r)
    step(final_e)
    norms_r.begin(mr[...], grad_r[...])
    step(final_e)
    norms_r.step()
    norms_r.step()
    norms_r.step()
    update(mr, vr, new_mr, new_vr, work_r, grad_r, norms_r)
    step(final_r)
    step(final_e)
    for _ in range(plan.n - 3):
        step(final_r, final_e)
    step(final_r)
    step(final_r)
    step(final_r)
    for task in gather_e + gather_r + final_e + final_r:
        assert task.t == -2
    for copy in used:
        copy.wait_send()


VMEM = pl.BlockSpec(memory_space=pltpu.VMEM)


def fused(plan, acts, hidden, grad_out, mr, me, vr, ve):
    rows, width = mr.shape
    n = plan.n
    cols = width // SLABS
    f32, bf16 = jnp.float32, jnp.bfloat16
    work = jax.ShapeDtypeStruct((2,) * n + (rows, width), bf16)
    shard = jax.ShapeDtypeStruct((rows, width), f32)
    slots = sum(plan.sizes[a] - 1 for a in AXES)
    half = [2 ** (n - t - 1) for t in range(n)]

    def stages(dtype):
        return [pltpu.VMEM((SLABS, b, rows, cols), dtype) for b in half]

    sems = pltpu.SemaphoreType.DMA
    out = pl.pallas_call(
        functools.partial(kernel, plan),
        out_shape=(jax.ShapeDtypeStruct(hidden.shape, bf16), work) + (shard,) * 4 + (work,) * 2,
        in_specs=[VMEM] * 7,
        out_specs=(VMEM,) * 8,
        scratch_shapes=[
            pltpu.VMEM((2,) * n + (rows, width), bf16),
            pltpu.VMEM((2**n, rows, width), f32),
            pltpu.VMEM((2**n, rows, width), f32),
            stages(f32), stages(f32), stages(bf16), stages(bf16), stages(bf16), stages(bf16),
            pltpu.VMEM((rows, width), f32),
            pltpu.VMEM((rows, width), f32),
            pltpu.VMEM((len(AXES) + 1, 8, 128), f32),
            pltpu.VMEM((len(AXES) + 1, 8, 128), f32),
            pltpu.VMEM((slots, 8, 128), f32),
            pltpu.VMEM((slots, 8, 128), f32),
            sems((4, n, SLABS)), sems((4, n, SLABS)),
            sems((2, n, SLABS)), sems((2, n, SLABS)),
            sems((2, slots)), sems((2, slots)),
        ],
        compiler_params=pltpu.CompilerParams(collective_id=0, has_side_effects=True),
        name="fused_step",
    )(acts, hidden, grad_out, mr, me, vr, ve)
    return [x.reshape(-1, width) if x.ndim > 2 else x for x in out]


def shards(
    plan, acts, saved_hidden, grad_out, master_reduce, master_expand,
    velocity_reduce, velocity_expand,
):
    inv_c = 1.0 / float(grad_out.shape[1]) ** 0.5
    f32 = jnp.float32
    grad_hidden, cur_reduce, *rest = fused(
        plan, acts, saved_hidden, grad_out, master_reduce, master_expand,
        velocity_reduce, velocity_expand,
    )
    back = lax.dot_general(
        grad_hidden, cur_reduce, (((1,), (1,)), ((), ())), preferred_element_type=f32
    )
    grad_in = (grad_out.astype(f32) + back * inv_c).astype(jnp.bfloat16)
    return (grad_in, *rest)


def solution(mesh):
    rows = P(AXES, None)
    return jax.shard_map(
        functools.partial(shards, Plan(mesh.shape)),
        mesh=mesh,
        in_specs=(rows,) * 7,
        out_specs=(rows,) * 5 + (P(), P()),
        check_vma=False,
    )
```
